32 devices in a mesh: groups: 2 (over y), graph: 16 (over z, x, core).
Axes of the slice: x: 2, y: 2, z: 4, core: 2. Of those that a mesh axis runs over, the one named last changes fastest.
Arguments:
- edge_state: bfloat16 [8192, 512], P(('groups', 'graph')), parts along dimension 0, may hold values from -6 to 6
- atom_state: bfloat16 [512, 256], P(('groups', 'graph')), parts along dimension 0, may hold values from -6 to 6
- atom_sends: int32 [4096], P(('groups', 'graph')), parts along dimension 0, may hold values from 0 to 15
- edge_source: int32 [8192], P(('groups', 'graph')), parts along dimension 0, may hold values from 0 to 127
- edge_target: int32 [8192], P(('groups', 'graph')), parts along dimension 0, may hold values from 0 to 15
- send_edges: int32 [262144], P(('groups', 'graph')), parts along dimension 0, may hold values from 0 to 255
- triplet_in: int32 [262144], P(('groups', 'graph')), parts along dimension 0, may hold values from 0 to 8191, as said below
- triplet_out: int32 [262144], P(('groups', 'graph')), parts along dimension 0, may hold values from 0 to 8191, as said below
- triplet_valid: int32 [262144], P(('groups', 'graph')), parts along dimension 0, may hold values 0 or 1
- triplet_basis: bfloat16 [16, 262144], P(None, ('groups', 'graph')), parts along dimension 1, may hold values from -6 to 6
- return_edges: int32 [262144], P(('groups', 'graph')), parts along dimension 0, may hold values from 0 to 255
- w_edge: bfloat16 [512, 512], replicated, may hold values from -0.25 to 0.25
- w_source: bfloat16 [256, 512], replicated, may hold values from -0.375 to 0.375
- w_down: bfloat16 [512, 64], replicated, may hold values from -0.25 to 0.25
- w_bilinear: bfloat16 [64, 1024], replicated, may hold values from -0.1875 to 0.1875
- w_up: bfloat16 [64, 512], replicated, may hold values from -0.125 to 0.125
- w_residual: bfloat16 [4, 512, 512], replicated, may hold values from -0.25 to 0.25
- w_atom: bfloat16 [512, 256], replicated, may hold values from -0.25 to 0.25
Outputs:
- edge_out: bfloat16 [8192, 512], P(('groups', 'graph')), parts along dimension 0
- atom_out: bfloat16 [512, 256], P(('groups', 'graph')), parts along dimension 0
The draws below stay inside these ranges and needn't reach their ends.
There are 2 independent parts, one for each index of `groups`. The reference program is written for one: setup_inputs(seed, part) draws one part's arguments, and reference() takes and returns one part's arrays. A program takes and returns all parts, laid end to end along the dimension named above; an argument that names none is the same for every part. Nothing has to cross between parts.
Inputs may be any that keep to these rules, and one draw needn't show every extreme that they name: `atom_sends`: entry d * 8 + c of a device's 128 entries is sent to device d. `send_edges`: entry t * 512 + c of a device's 8192 entries is sent to tile t. `triplet_in`: triplet j of a tile reads a received slot in the same aligned block of 512 slots as j. `triplet_out`: slot d * 512 + c of a tile is returned to device d; triplet j of a tile adds to a slot in the same aligned block of 512 slots as j. `return_edges`: entry t * 512 + c of a device's 8192 entries belongs to the slot that tile t returns in place c.
All inputs are finite; a program needn't handle non-finite values. No bound on the sum of `triplet_valid` on one device may be relied on, other than what follows from the above.
Results may differ from the reference program's by a relative error of at most 0.0095.
Values may be sent and summed in bfloat16 or wider, within the bound.
A program may use at most 64 MiB of HBM per device.

```python
import jax
import jax.numpy as jnp
from jax import lax

DE = 512
DA = 256
DP = 64
NB = 16
E_DEV = 256
TPE = 32
WIN = 512
ATOM_DEV = 16
EDGES = 4096
ATOMS = 256
TRIP_DEV = 8192
TRIPLETS = 131072
CAP = 512
ASLOTS = 128
CAP_A = 8
ASENDS = 2048
N_GRAPH = 16


def block_slots(key):
    positions = jnp.arange(TRIPLETS, dtype=jnp.int32) % TRIP_DEV
    starts = positions // WIN * WIN
    return starts + jax.random.randint(key, (TRIPLETS,), 0, WIN, dtype=jnp.int32)


def draw_triplet_in(key, part):
    return block_slots(jax.random.fold_in(key, 101))


def draw_triplet_out(key, part):
    return block_slots(jax.random.fold_in(key, 202))


def touch_ends(entries, key, smallest, high):
    longest = entries.shape.index(max(entries.shape))
    spots = []
    for shift in (0, 1):
        where = [jax.random.randint(jax.random.fold_in(key, axis), (), 0, length) for axis, length in enumerate(entries.shape)]
        where[longest] = (where[longest] + shift) % entries.shape[longest]
        spots.append(tuple(where))
    return entries.at[spots[0]].set(smallest).at[spots[1]].set(high)


def block_levels(own_key, dims, cuts, low, top_value):
    factor_of, own = 1.0, jax.random.fold_in(own_key, 6)
    for dim, shards_of in cuts:
        steps = jnp.exp(jax.random.uniform(jax.random.fold_in(own, dim), (shards_of,), jnp.float32, low / len(cuts), top_value / len(cuts)))
        factor_of = factor_of * jnp.repeat(steps, dims[dim] // shards_of).reshape([-1 if axis == dim else 1 for axis in range(len(dims))])
    return factor_of


def bell_draw(rng, dims, scale, most, pieces=(), kind=jnp.bfloat16):
    gain = block_levels(rng, dims, pieces, -0.22, 0.18) if pieces else 1.0
    entries = jax.random.normal(rng, dims, jnp.float32) * scale * gain
    return jnp.minimum(jnp.maximum(entries, -most), most).astype(kind)


def setup_inputs(seed: int = 0, part: int = 0) -> dict:
    streams_of = jax.random.split(jax.random.key(seed), 19)
    own_keys = jax.random.split(jax.random.fold_in(streams_of[18], part), 19)
    return {
        "edge_state": bell_draw(own_keys[0], (EDGES, DE), 1.0, 6.0, ((0, 16),)),
        "atom_state": bell_draw(own_keys[1], (ATOMS, DA), 1.0, 6.0, ((0, 16),)),
        "atom_sends": touch_ends(jax.random.randint(own_keys[2], (ASENDS,), 0, ATOM_DEV), jax.random.fold_in(own_keys[2], 1), 0, ATOM_DEV - 1).astype(jnp.int32),
        "edge_source": touch_ends(jax.random.randint(own_keys[3], (EDGES,), 0, ASLOTS), jax.random.fold_in(own_keys[3], 1), 0, ASLOTS - 1).astype(jnp.int32),
        "edge_target": touch_ends(jax.random.randint(own_keys[4], (EDGES,), 0, ATOM_DEV), jax.random.fold_in(own_keys[4], 1), 0, ATOM_DEV - 1).astype(jnp.int32),
        "send_edges": touch_ends(jax.random.randint(own_keys[5], (TRIPLETS,), 0, E_DEV), jax.random.fold_in(own_keys[5], 1), 0, E_DEV - 1).astype(jnp.int32),
        "triplet_in": draw_triplet_in(jax.random.fold_in(jax.random.fold_in(streams_of[18], part), 71), part),
        "triplet_out": draw_triplet_out(jax.random.fold_in(jax.random.fold_in(streams_of[18], part), 71), part),
        "triplet_valid": touch_ends((jax.random.randint(own_keys[8], (TRIPLETS,), 0, 4) < 3).astype(jnp.int32), jax.random.fold_in(own_keys[8], 1), 0, 1),
        "triplet_basis": bell_draw(own_keys[9], (NB, TRIPLETS), 1.0, 6.0, ((1, 16),)),
        "return_edges": touch_ends(jax.random.randint(own_keys[10], (TRIPLETS,), 0, E_DEV), jax.random.fold_in(own_keys[10], 1), 0, E_DEV - 1).astype(jnp.int32),
        "w_edge": bell_draw(streams_of[11], (DE, DE), DE ** -0.5, 0.25),
        "w_source": bell_draw(streams_of[12], (DA, DE), DA ** -0.5, 0.375),
        "w_down": bell_draw(streams_of[13], (DE, DP), DE ** -0.5, 0.25),
        "w_bilinear": bell_draw(streams_of[14], (DP, NB * DP), (DP * NB) ** -0.5, 0.1875),
        "w_up": bell_draw(streams_of[15], (DP, DE), (DP * TPE) ** -0.5, 0.125),
        "w_residual": bell_draw(streams_of[16], (4, DE, DE), DE ** -0.5, 0.25),
        "w_atom": bell_draw(streams_of[17], (DE, DA), DE ** -0.5, 0.25),
    }


inv_root = 0.7071067811865476


def matmul(left, right):
    return jnp.dot(left, right, preferred_element_type=jnp.float32)


def bilinear_terms(inputs_x, coeffs, keeps, w_bilinear):
    expanded = matmul(inputs_x, w_bilinear)
    expanded = expanded.reshape(inputs_x.shape[0], coeffs.shape[0], -1)
    mixed = jnp.einsum("tkd,kt->td", expanded, coeffs.astype(jnp.float32))
    return mixed * keeps.astype(jnp.float32)[:, None]


def slot_table(indices, peer_count, width, shift):
    offsets = (jnp.arange(peer_count, dtype=jnp.int32) * shift)[:, None, None]
    shaped = indices.reshape(peer_count, peer_count, width) + offsets
    return jnp.transpose(shaped, (1, 0, 2)).reshape(peer_count, peer_count * width)


def reference(edge_state, atom_state, atom_sends, edge_source, edge_target, send_edges, triplet_in, triplet_out, triplet_valid, triplet_basis, return_edges, w_edge, w_source, w_down, w_bilinear, w_up, w_residual, w_atom):
    peer_count = N_GRAPH
    atom_slots = slot_table(atom_sends, peer_count, CAP_A, ATOM_DEV)
    source_ids = jnp.take_along_axis(atom_slots, edge_source.reshape(peer_count, E_DEV), axis=1).reshape(-1)
    src_rows = atom_state[source_ids]
    pre_act = matmul(edge_state, w_edge) + matmul(src_rows, w_source)
    activated = jax.nn.silu(pre_act).astype(jnp.bfloat16)
    projected = jax.nn.silu(matmul(activated, w_down)).astype(jnp.bfloat16)
    edge_slots = slot_table(send_edges, peer_count, CAP, E_DEV)
    back_slots = slot_table(return_edges, peer_count, CAP, E_DEV)

    def tile_work(operands):
        slot_ids, local_in, local_out, keeps, coeffs = operands
        inputs_x = projected[slot_ids[local_in]]
        mixed = bilinear_terms(inputs_x, coeffs, keeps, w_bilinear)
        summed = jnp.zeros((TRIP_DEV, DP), jnp.float32).at[local_out].add(mixed)
        return summed.astype(jnp.bfloat16)

    basis_tiles = jnp.transpose(triplet_basis.reshape(NB, peer_count, TRIP_DEV), (1, 0, 2))
    slot_sums = lax.map(tile_work, (edge_slots, triplet_in.reshape(peer_count, TRIP_DEV), triplet_out.reshape(peer_count, TRIP_DEV), triplet_valid.reshape(peer_count, TRIP_DEV), basis_tiles))
    aggregate = jnp.zeros((EDGES, DP), jnp.float32).at[back_slots.reshape(-1)].add(slot_sums.reshape(-1, DP).astype(jnp.float32))
    aggregate = aggregate.astype(jnp.bfloat16)
    update = jax.nn.silu(matmul(aggregate, w_up))
    base = ((edge_state.astype(jnp.float32) + activated.astype(jnp.float32)) * inv_root).astype(jnp.bfloat16)
    inner_one = jax.nn.silu(matmul(base, w_residual[0])).astype(jnp.bfloat16)
    middle = ((base.astype(jnp.float32) + jax.nn.silu(matmul(inner_one, w_residual[1]))) * inv_root).astype(jnp.bfloat16)
    inner_two = jax.nn.silu(matmul(middle, w_residual[2])).astype(jnp.bfloat16)
    chain = (middle.astype(jnp.float32) + jax.nn.silu(matmul(inner_two, w_residual[3]))) * inv_root
    edge_out = (chain + update).astype(jnp.bfloat16)
    contrib = matmul(edge_out, w_atom).astype(jnp.bfloat16)
    targets = edge_target + (jnp.arange(EDGES, dtype=jnp.int32) // E_DEV) * ATOM_DEV
    atom_sum = jnp.zeros((ATOMS, DA), jnp.float32).at[targets].add(contrib.astype(jnp.float32))
    atom_out = (atom_state.astype(jnp.float32) + jax.nn.silu(0.25 * atom_sum)).astype(jnp.bfloat16)
    return edge_out, atom_out
```

```python
import functools

import jax
import jax.numpy as jnp
from jax import lax
from jax.experimental import pallas as pl
from jax.experimental.pallas import tpu as pltpu
from jax.sharding import PartitionSpec as P

WIN = 512


inv_root = 0.7071067811865476


def matmul(left, right):
    return jnp.dot(left, right, preferred_element_type=jnp.float32)


def pick_rows(indices, table):
    chooser = (indices[:, None] == jnp.arange(table.shape[0], dtype=jnp.int32)[None, :]).astype(
        table.dtype
    )
    return matmul(chooser, table).astype(table.dtype)


def bilinear_terms(inputs_x, coeffs, keeps, w_bilinear):
    expanded = matmul(inputs_x, w_bilinear)
    expanded = expanded.reshape(inputs_x.shape[0], coeffs.shape[0], -1)
    mixed = jnp.einsum("tkd,kt->td", expanded, coeffs.astype(jnp.float32))
    return mixed * keeps.astype(jnp.float32)[:, None]


def tile_sums(slot_rows, local_in, local_out, keeps, coeffs, w_bilinear):
    trip_count = slot_rows.shape[0]
    block_size = WIN
    block_count = trip_count // block_size
    basis_rows = coeffs.shape[0]
    block_iota = jnp.arange(block_size, dtype=jnp.int32)

    def one_block(operands):
        rows_blk, in_blk, out_blk, keep_blk, coef_blk = operands
        in_hot = ((in_blk % block_size)[:, None] == block_iota[None, :]).astype(jnp.bfloat16)
        inputs_x = matmul(in_hot, rows_blk).astype(jnp.bfloat16)
        mixed = bilinear_terms(inputs_x, coef_blk, keep_blk, w_bilinear)
        out_hot = (block_iota[:, None] == (out_blk % block_size)[None, :]).astype(jnp.float32)
        return jnp.dot(
            out_hot, mixed, precision=lax.Precision.HIGHEST, preferred_element_type=jnp.float32
        )

    shaped_coeffs = jnp.transpose(coeffs.reshape(basis_rows, block_count, block_size), (1, 0, 2))
    summed = lax.map(
        one_block,
        (
            slot_rows.reshape(block_count, block_size, -1),
            local_in.reshape(block_count, block_size),
            local_out.reshape(block_count, block_size),
            keeps.reshape(block_count, block_size),
            shaped_coeffs,
        ),
    )
    return summed.reshape(trip_count, -1).astype(jnp.bfloat16)


def plain_on_device(
    edge_state,
    atom_state,
    atom_sends,
    edge_source,
    edge_target,
    send_edges,
    triplet_in,
    triplet_out,
    triplet_valid,
    triplet_basis,
    return_edges,
    w_edge,
    w_source,
    w_down,
    w_bilinear,
    w_up,
    w_residual,
    w_atom,
):
    edge_count = edge_state.shape[0]
    atom_count = atom_state.shape[0]
    arrived_atoms = lax.all_to_all(
        pick_rows(atom_sends, atom_state), "graph", split_axis=0, concat_axis=0, tiled=True
    )
    src_rows = pick_rows(edge_source, arrived_atoms)
    pre_act = matmul(edge_state, w_edge) + matmul(src_rows, w_source)
    activated = jax.nn.silu(pre_act).astype(jnp.bfloat16)
    projected = jax.nn.silu(matmul(activated, w_down)).astype(jnp.bfloat16)
    slot_rows = lax.all_to_all(
        pick_rows(send_edges, projected), "graph", split_axis=0, concat_axis=0, tiled=True
    )
    slot_sums = tile_sums(
        slot_rows, triplet_in, triplet_out, triplet_valid, triplet_basis, w_bilinear
    )
    returned = lax.all_to_all(slot_sums, "graph", split_axis=0, concat_axis=0, tiled=True)
    back_hot = (jnp.arange(edge_count, dtype=jnp.int32)[:, None] == return_edges[None, :]).astype(
        jnp.bfloat16
    )
    aggregate = matmul(back_hot, returned)
    update = jax.nn.silu(matmul(aggregate.astype(jnp.bfloat16), w_up))
    base = ((edge_state.astype(jnp.float32) + activated.astype(jnp.float32)) * inv_root).astype(
        jnp.bfloat16
    )
    inner_one = jax.nn.silu(matmul(base, w_residual[0])).astype(jnp.bfloat16)
    middle = (
        (base.astype(jnp.float32) + jax.nn.silu(matmul(inner_one, w_residual[1]))) * inv_root
    ).astype(jnp.bfloat16)
    inner_two = jax.nn.silu(matmul(middle, w_residual[2])).astype(jnp.bfloat16)
    chain = (middle.astype(jnp.float32) + jax.nn.silu(matmul(inner_two, w_residual[3]))) * inv_root
    edge_out = (chain + update).astype(jnp.bfloat16)
    contrib = matmul(edge_out, w_atom).astype(jnp.bfloat16)
    one_hot = (edge_target[None, :] == jnp.arange(atom_count, dtype=jnp.int32)[:, None]).astype(
        jnp.bfloat16
    )
    atom_sum = matmul(one_hot, contrib)
    atom_out = (atom_state.astype(jnp.float32) + jax.nn.silu(0.25 * atom_sum)).astype(jnp.bfloat16)
    return (edge_out, atom_out)


def silu(value):
    return value / (1.0 + jnp.exp(-value))


def dot_at(left, right, left_dim, right_dim):
    return lax.dot_general(
        left, right, (((left_dim,), (right_dim,)), ((), ())), preferred_element_type=jnp.float32
    )


def hot_columns(row_count, indices):
    rows = lax.broadcasted_iota(jnp.int32, (row_count, indices.shape[1]), 0)
    return jnp.where(rows == indices, 1.0, 0.0).astype(jnp.bfloat16)


def front_kernel(
    n,
    atom_ref,
    asend_ref,
    source_ref,
    edge_hbm,
    ends_hbm,
    basis_hbm,
    w_edge_hbm,
    w_source_hbm,
    w_down_hbm,
    w_res_hbm,
    proj_ref,
    chain_ref,
    ends_out,
    basis_out,
    edge_v,
    w_edge_v,
    w_source_v,
    w_down_v,
    w_res_v,
    atoms_out,
    atoms_in,
    load_sem,
    own_sem,
    send_sem,
    recv_sem,
):
    me = lax.axis_index("graph")
    cap = ends_out.shape[2]
    loads = [
        pltpu.make_async_copy(src, dst, load_sem.at[i])
        for i, (src, dst) in enumerate(
            (
                (edge_hbm, edge_v),
                (w_edge_hbm, w_edge_v),
                (w_source_hbm, w_source_v),
                (w_down_hbm, w_down_v),
                (w_res_hbm, w_res_v),
            )
        )
    ]
    for load in loads:
        load.start()

    barrier = pltpu.get_barrier_semaphore()
    for step in range(1, n):
        pl.semaphore_signal(
            barrier,
            inc=1,
            device_id={"graph": lax.rem(me + step, n)},
            device_id_type=pl.DeviceIdType.MESH,
        )
    picked = dot_at(hot_columns(atom_ref.shape[0], asend_ref[...]), atom_ref[...], 0, 0)
    atoms_out[...] = picked.reshape(atoms_out.shape).astype(jnp.bfloat16)
    pl.semaphore_wait(barrier, n - 1)

    def parts(peer):
        lanes = pl.ds(pl.multiple_of(peer * cap, cap), cap)
        return (
            (atoms_out.at[peer], atoms_in.at[me]),
            (ends_hbm.at[peer], ends_out.at[me]),
            (basis_hbm.at[:, lanes], basis_out.at[me]),
        )

    remote = [[], [], []]
    local = []
    for kind in range(3):
        for step in range(1, n):
            peer = lax.rem(me + step, n)
            src, dst = parts(peer)[kind]
            copy = pltpu.make_async_remote_copy(
                src_ref=src,
                dst_ref=dst,
                send_sem=send_sem.at[kind, step],
                recv_sem=recv_sem.at[kind, step],
                device_id={"graph": peer},
                device_id_type=pl.DeviceIdType.MESH,
            )
            copy.start()
            remote[kind].append(copy)
        src, dst = parts(me)[kind]
        copy = pltpu.make_async_copy(src, dst, own_sem.at[kind])
        copy.start()
        local.append(copy)

    loads[0].wait()
    loads[1].wait()
    edge = edge_v[...]
    pre_act = matmul(edge, w_edge_v[...])
    pick = hot_columns(atoms_in.shape[0] * atoms_in.shape[1], source_ref[...])
    loads[2].wait()
    loads[3].wait()
    for copy in remote[0]:
        copy.wait_recv()
    local[0].wait()
    arrived = atoms_in[...].astype(jnp.float32).reshape(pick.shape[0], -1).astype(jnp.bfloat16)
    src_rows = dot_at(pick, arrived, 0, 0).astype(jnp.bfloat16)
    activated = silu(pre_act + matmul(src_rows, w_source_v[...])).astype(jnp.bfloat16)
    proj_ref[...] = silu(matmul(activated, w_down_v[...])).astype(jnp.bfloat16)
    loads[4].wait()
    base = ((edge.astype(jnp.float32) + activated.astype(jnp.float32)) * inv_root).astype(
        jnp.bfloat16
    )
    inner_one = silu(matmul(base, w_res_v[0])).astype(jnp.bfloat16)
    middle = ((base.astype(jnp.float32) + silu(matmul(inner_one, w_res_v[1]))) * inv_root).astype(
        jnp.bfloat16
    )
    inner_two = silu(matmul(middle, w_res_v[2])).astype(jnp.bfloat16)
    chain_ref[...] = (middle.astype(jnp.float32) + silu(matmul(inner_two, w_res_v[3]))) * inv_root
    for kind in (1, 2):
        for copy in remote[kind]:
            copy.wait_recv()
        local[kind].wait()
    for kind in range(3):
        for copy in remote[kind]:
            copy.wait_send()


def look_up(table, indices):
    width = 128
    found = []
    for start in range(0, indices.shape[1], width):
        wanted = indices[:, start : start + width]
        lane = lax.rem(wanted, width)
        chunk_of = wanted // width
        value = jnp.zeros_like(wanted)
        for chunk in range(table.shape[1] // width):
            part = jnp.take_along_axis(
                table[:, chunk * width : (chunk + 1) * width], lane, axis=1, mode="promise_in_bounds"
            )
            value = jnp.where(chunk_of == chunk, part, value)
        found.append(value)
    return jnp.concatenate(found, axis=1)


def triplet_kernel(
    n,
    proj_ref,
    chain_ref,
    ends_ref,
    basis_ref,
    send_ref,
    return_ref,
    target_ref,
    atom_ref,
    w_bilinear_ref,
    w_up_ref,
    w_atom_ref,
    edge_out_ref,
    atom_out_ref,
    table_v,
    in_v,
    out_v,
    expand_v,
    sum_v,
):
    edge_count, width = proj_ref.shape
    basis_count, cap = basis_ref.shape[1:]
    table_v[...] = dot_at(w_bilinear_ref[...], proj_ref[...], 0, 1).astype(jnp.bfloat16)
    for start in range(0, n, 8):
        some = slice(start, start + 8)
        in_v[some] = look_up(send_ref[some], ends_ref[some, 0, :])
        out_v[some] = look_up(return_ref[some], ends_ref[some, 1, :])
    sum_v[...] = jnp.zeros_like(sum_v)

    def one_tile(tile, carry):
        expand_v[...] = matmul(table_v[...], hot_columns(edge_count, in_v[pl.ds(tile, 1), :]))
        coeffs = basis_ref[tile].astype(jnp.float32)
        mixed = jnp.zeros((width, cap), jnp.float32)
        for k in range(basis_count):
            mixed = mixed + coeffs[k : k + 1, :] * expand_v[k * width : (k + 1) * width, :]
        out_hot = hot_columns(edge_count, out_v[pl.ds(tile, 1), :])
        sum_v[...] += dot_at(mixed.astype(jnp.bfloat16), out_hot, 1, 1)
        return carry

    lax.fori_loop(0, n, one_tile, 0, unroll=2)
    aggregate = sum_v[...].T.astype(jnp.bfloat16)
    update = silu(matmul(aggregate, w_up_ref[...]))
    edge_out = (chain_ref[...] + update).astype(jnp.bfloat16)
    edge_out_ref[...] = edge_out
    contrib = matmul(edge_out, w_atom_ref[...]).astype(jnp.bfloat16)
    atom_sum = matmul(hot_columns(atom_ref.shape[0], target_ref[...]), contrib)
    atom_out_ref[...] = (atom_ref[...].astype(jnp.float32) + silu(0.25 * atom_sum)).astype(
        jnp.bfloat16
    )


def on_device(
    n,
    edge_state,
    atom_state,
    atom_sends,
    edge_source,
    edge_target,
    send_edges,
    triplet_in,
    triplet_out,
    triplet_valid,
    triplet_basis,
    return_edges,
    w_edge,
    w_source,
    w_down,
    w_bilinear,
    w_up,
    w_residual,
    w_atom,
):
    cap = triplet_in.shape[0] // n
    if cap % WIN or n % 8:
        return plain_on_device(
            edge_state,
            atom_state,
            atom_sends,
            edge_source,
            edge_target,
            send_edges,
            triplet_in,
            triplet_out,
            triplet_valid,
            triplet_basis,
            return_edges,
            w_edge,
            w_source,
            w_down,
            w_bilinear,
            w_up,
            w_residual,
            w_atom,
        )
    edge_count, edge_width = edge_state.shape
    atom_count, atom_width = atom_state.shape
    basis_count = triplet_basis.shape[0]
    width = w_down.shape[1]
    slots = atom_sends.shape[0] // n
    ends = jnp.stack(
        [(triplet_in % cap).reshape(n, cap), (triplet_out % cap).reshape(n, cap)], axis=1
    )
    basis = triplet_basis * triplet_valid.astype(triplet_basis.dtype)[None, :]
    vmem = pl.BlockSpec(memory_space=pltpu.VMEM)
    hbm = pl.BlockSpec(memory_space=pl.ANY)
    bf16 = jnp.bfloat16
    projected, chain, my_ends, my_basis = pl.pallas_call(
        functools.partial(front_kernel, n),
        out_shape=(
            jax.ShapeDtypeStruct((edge_count, width), bf16),
            jax.ShapeDtypeStruct((edge_count, edge_width), jnp.float32),
            jax.ShapeDtypeStruct((n, 2, cap), jnp.int32),
            jax.ShapeDtypeStruct((n, basis_count, cap), bf16),
        ),
        in_specs=[vmem] * 3 + [hbm] * 7,
        out_specs=(vmem, vmem, vmem, vmem),
        scratch_shapes=[
            pltpu.VMEM(edge_state.shape, bf16),
            pltpu.VMEM(w_edge.shape, bf16),
            pltpu.VMEM(w_source.shape, bf16),
            pltpu.VMEM(w_down.shape, bf16),
            pltpu.VMEM(w_residual.shape, bf16),
            pltpu.VMEM((n, slots, atom_width), bf16),
            pltpu.VMEM((n, slots, atom_width), bf16),
            pltpu.SemaphoreType.DMA((5,)),
            pltpu.SemaphoreType.DMA((3,)),
            pltpu.SemaphoreType.DMA((3, n)),
            pltpu.SemaphoreType.DMA((3, n)),
        ],
        compiler_params=pltpu.CompilerParams(collective_id=0, has_side_effects=True),
        name="front",
    )(
        atom_state,
        atom_sends.reshape(1, -1),
        edge_source.reshape(1, -1),
        edge_state,
        ends,
        basis,
        w_edge,
        w_source,
        w_down,
        w_residual,
    )
    return pl.pallas_call(
        functools.partial(triplet_kernel, n),
        out_shape=(
            jax.ShapeDtypeStruct((edge_count, edge_width), bf16),
            jax.ShapeDtypeStruct((atom_count, atom_width), bf16),
        ),
        in_specs=[vmem] * 11,
        out_specs=(vmem, vmem),
        scratch_shapes=[
            pltpu.VMEM((basis_count * width, edge_count), bf16),
            pltpu.VMEM((n, cap), jnp.int32),
            pltpu.VMEM((n, cap), jnp.int32),
            pltpu.VMEM((basis_count * width, cap), jnp.float32),
            pltpu.VMEM((width, edge_count), jnp.float32),
        ],
        name="triplets",
    )(
        projected,
        chain,
        my_ends,
        my_basis,
        send_edges.reshape(n, cap),
        return_edges.reshape(n, cap),
        edge_target.reshape(1, -1),
        atom_state,
        w_bilinear,
        w_up,
        w_atom,
    )


def solution(mesh):
    placed = (
        P(("groups", "graph"), None),
        P(("groups", "graph"), None),
        P(("groups", "graph")),
        P(("groups", "graph")),
        P(("groups", "graph")),
        P(("groups", "graph")),
        P(("groups", "graph")),
        P(("groups", "graph")),
        P(("groups", "graph")),
        P(None, ("groups", "graph")),
        P(("groups", "graph")),
        P(),
        P(),
        P(),
        P(),
        P(),
        P(),
        P(),
    )
    return jax.shard_map(
        functools.partial(on_device, mesh.shape["graph"]),
        mesh=mesh,
        in_specs=placed,
        out_specs=(P(("groups", "graph"), None), P(("groups", "graph"), None)),
        check_vma=False,
    )
```

```python
import functools

import jax
import jax.numpy as jnp
from jax import lax
from jax.experimental import pallas as pl
from jax.experimental.pallas import tpu as pltpu
from jax.sharding import PartitionSpec as P

WIN = 512


inv_root = 0.7071067811865476


def matmul(left, right):
    return jnp.dot(left, right, preferred_element_type=jnp.float32)


def pick_rows(indices, table):
    chooser = (indices[:, None] == jnp.arange(table.shape[0], dtype=jnp.int32)[None, :]).astype(
        table.dtype
    )
    return matmul(chooser, table).astype(table.dtype)


def bilinear_terms(inputs_x, coeffs, keeps, w_bilinear):
    expanded = matmul(inputs_x, w_bilinear)
    expanded = expanded.reshape(inputs_x.shape[0], coeffs.shape[0], -1)
    mixed = jnp.einsum("tkd,kt->td", expanded, coeffs.astype(jnp.float32))
    return mixed * keeps.astype(jnp.float32)[:, None]


def tile_sums(slot_rows, local_in, local_out, keeps, coeffs, w_bilinear):
    trip_count = slot_rows.shape[0]
    block_size = WIN
    block_count = trip_count // block_size
    basis_rows = coeffs.shape[0]
    block_iota = jnp.arange(block_size, dtype=jnp.int32)

    def one_block(operands):
        rows_blk, in_blk, out_blk, keep_blk, coef_blk = operands
        in_hot = ((in_blk % block_size)[:, None] == block_iota[None, :]).astype(jnp.bfloat16)
        inputs_x = matmul(in_hot, rows_blk).astype(jnp.bfloat16)
        mixed = bilinear_terms(inputs_x, coef_blk, keep_blk, w_bilinear)
        out_hot = (block_iota[:, None] == (out_blk % block_size)[None, :]).astype(jnp.float32)
        return jnp.dot(
            out_hot, mixed, precision=lax.Precision.HIGHEST, preferred_element_type=jnp.float32
        )

    shaped_coeffs = jnp.transpose(coeffs.reshape(basis_rows, block_count, block_size), (1, 0, 2))
    summed = lax.map(
        one_block,
        (
            slot_rows.reshape(block_count, block_size, -1),
            local_in.reshape(block_count, block_size),
            local_out.reshape(block_count, block_size),
            keeps.reshape(block_count, block_size),
            shaped_coeffs,
        ),
    )
    return summed.reshape(trip_count, -1).astype(jnp.bfloat16)


def plain_on_device(
    edge_state,
    atom_state,
    atom_sends,
    edge_source,
    edge_target,
    send_edges,
    triplet_in,
    triplet_out,
    triplet_valid,
    triplet_basis,
    return_edges,
    w_edge,
    w_source,
    w_down,
    w_bilinear,
    w_up,
    w_residual,
    w_atom,
):
    edge_count = edge_state.shape[0]
    atom_count = atom_state.shape[0]
    arrived_atoms = lax.all_to_all(
        pick_rows(atom_sends, atom_state), "graph", split_axis=0, concat_axis=0, tiled=True
    )
    src_rows = pick_rows(edge_source, arrived_atoms)
    pre_act = matmul(edge_state, w_edge) + matmul(src_rows, w_source)
    activated = jax.nn.silu(pre_act).astype(jnp.bfloat16)
    projected = jax.nn.silu(matmul(activated, w_down)).astype(jnp.bfloat16)
    slot_rows = lax.all_to_all(
        pick_rows(send_edges, projected), "graph", split_axis=0, concat_axis=0, tiled=True
    )
    slot_sums = tile_sums(
        slot_rows, triplet_in, triplet_out, triplet_valid, triplet_basis, w_bilinear
    )
    returned = lax.all_to_all(slot_sums, "graph", split_axis=0, concat_axis=0, tiled=True)
    back_hot = (jnp.arange(edge_count, dtype=jnp.int32)[:, None] == return_edges[None, :]).astype(
        jnp.bfloat16
    )
    aggregate = matmul(back_hot, returned)
    update = jax.nn.silu(matmul(aggregate.astype(jnp.bfloat16), w_up))
    base = ((edge_state.astype(jnp.float32) + activated.astype(jnp.float32)) * inv_root).astype(
        jnp.bfloat16
    )
    inner_one = jax.nn.silu(matmul(base, w_residual[0])).astype(jnp.bfloat16)
    middle = (
        (base.astype(jnp.float32) + jax.nn.silu(matmul(inner_one, w_residual[1]))) * inv_root
    ).astype(jnp.bfloat16)
    inner_two = jax.nn.silu(matmul(middle, w_residual[2])).astype(jnp.bfloat16)
    chain = (middle.astype(jnp.float32) + jax.nn.silu(matmul(inner_two, w_residual[3]))) * inv_root
    edge_out = (chain + update).astype(jnp.bfloat16)
    contrib = matmul(edge_out, w_atom).astype(jnp.bfloat16)
    one_hot = (edge_target[None, :] == jnp.arange(atom_count, dtype=jnp.int32)[:, None]).astype(
        jnp.bfloat16
    )
    atom_sum = matmul(one_hot, contrib)
    atom_out = (atom_state.astype(jnp.float32) + jax.nn.silu(0.25 * atom_sum)).astype(jnp.bfloat16)
    return (edge_out, atom_out)


def silu(value):
    return value / (1.0 + jnp.exp(-value))


def dot_at(left, right, left_dim, right_dim):
    return lax.dot_general(
        left, right, (((left_dim,), (right_dim,)), ((), ())), preferred_element_type=jnp.float32
    )


def hot_columns(row_count, indices):
    rows = lax.broadcasted_iota(jnp.int32, (row_count, indices.shape[1]), 0)
    return jnp.where(rows == indices, 1.0, 0.0).astype(jnp.bfloat16)


def partner(me, step, n):
    peer = me
    bit = 1
    while bit < n:
        mine = lax.rem(lax.div(me, bit), 2)
        flip = (step // bit) % 2 if isinstance(step, int) else lax.rem(lax.div(step, bit), 2)
        peer = peer + flip * (1 - 2 * mine) * bit
        bit *= 2
    return peer


def look_up(table, indices):
    lanes = 128
    found = []
    for start in range(0, indices.shape[1], lanes):
        wanted = jnp.broadcast_to(indices[:, start : start + lanes], (8, lanes))
        lane = wanted & (lanes - 1)
        value = jnp.zeros_like(wanted)
        for first in range(0, table.shape[1], lanes):
            part = jnp.take_along_axis(
                jnp.broadcast_to(table[:, first : first + lanes], (8, lanes)),
                lane,
                axis=1,
                mode="promise_in_bounds",
            )
            value = jnp.where(wanted - lane == first, part, value)
        found.append(value)
    return jnp.concatenate(found, axis=1)


def hot_from(row_count, eight_rows):
    rows = lax.broadcasted_iota(jnp.int32, (row_count, eight_rows.shape[1]), 0)
    spread = jnp.concatenate([eight_rows] * (row_count // 8), axis=0)
    return jnp.where(rows == spread, 1.0, 0.0).astype(jnp.bfloat16)


def block_kernel(n, loaded, *refs):
    sources = refs[:loaded]
    in_hbm, out_hbm, valid_hbm, basis_hbm = refs[loaded : loaded + 4]
    edge_out_ref, atom_out_ref = refs[loaded + 4 : loaded + 6]
    held = refs[loaded + 6 : 2 * loaded + 6]
    (
        in_v,
        out_v,
        valid_v,
        basis_v,
        atoms_out,
        atoms_in,
        chain_v,
        table_v,
        expand_v,
        sum_v,
        load_sem,
        send_sem,
        recv_sem,
    ) = refs[2 * loaded + 6 :]
    (
        atom_v,
        asend_v,
        edge_v,
        w_edge_v,
        source_v,
        w_source_v,
        w_down_v,
        w_bilinear_v,
        w_res_v,
        send_v,
        return_v,
        target_v,
        w_up_v,
        w_atom_v,
    ) = held
    me = lax.axis_index("graph")
    cap = in_v.shape[2]
    edge_count = edge_v.shape[0]
    width = w_down_v.shape[0]
    basis_count = basis_v.shape[1]

    barrier = pltpu.get_barrier_semaphore()
    for step in range(1, n):
        pl.semaphore_signal(
            barrier,
            inc=1,
            device_id={"graph": partner(me, step, n)},
            device_id_type=pl.DeviceIdType.MESH,
        )
    loads = [
        pltpu.make_async_copy(src, dst, load_sem.at[i])
        for i, (src, dst) in enumerate(zip(sources, held))
    ]
    for load in loads:
        load.start()
    loads[0].wait()
    loads[1].wait()
    picked = dot_at(hot_columns(atom_v.shape[0], asend_v[...]), atom_v[...], 0, 0)
    atoms_out[...] = picked.reshape(atoms_out.shape).astype(jnp.bfloat16)
    pl.semaphore_wait(barrier, n - 1)

    def parts(peer):
        lanes = pl.ds(pl.multiple_of(peer * cap, cap), cap)
        return (
            (atoms_out.at[peer], atoms_in.at[me]),
            (in_hbm.at[peer], in_v.at[me]),
            (out_hbm.at[peer], out_v.at[me]),
            (valid_hbm.at[peer], valid_v.at[me]),
            (basis_hbm.at[:, lanes], basis_v.at[me]),
        )

    sent = []
    for kinds in ((0,), (1, 2, 3, 4)):
        for step in range(n):
            peer = partner(me, step, n)
            for kind in kinds:
                src, dst = parts(peer)[kind]
                if step == 0:
                    copy = pltpu.make_async_copy(src, dst, recv_sem.at[kind, step])
                else:
                    copy = pltpu.make_async_remote_copy(
                        src_ref=src,
                        dst_ref=dst,
                        send_sem=send_sem.at[kind, step],
                        recv_sem=recv_sem.at[kind, step],
                        device_id={"graph": peer},
                        device_id_type=pl.DeviceIdType.MESH,
                    )
                    sent.append(copy)
                copy.start()

    def arrive(kind, buffer, step, peer):
        pltpu.make_async_copy(buffer.at[peer], buffer.at[peer], recv_sem.at[kind, step]).wait()

    for load in loads[2:7]:
        load.wait()
    edge = edge_v[...]
    pre_act = matmul(edge, w_edge_v[...])
    pick = hot_columns(atoms_in.shape[0] * atoms_in.shape[1], source_v[...])
    for step in range(n):
        arrive(0, atoms_in, step, partner(me, step, n))
    arrived = atoms_in[...].astype(jnp.float32).reshape(pick.shape[0], -1).astype(jnp.bfloat16)
    src_rows = dot_at(pick, arrived, 0, 0).astype(jnp.bfloat16)
    activated = silu(pre_act + matmul(src_rows, w_source_v[...])).astype(jnp.bfloat16)
    projected = silu(dot_at(activated, w_down_v[...], 1, 1)).astype(jnp.bfloat16)
    for load in loads[7:]:
        load.wait()
    table_v[...] = dot_at(w_bilinear_v[...], projected, 0, 1).astype(jnp.bfloat16)
    base = ((edge.astype(jnp.float32) + activated.astype(jnp.float32)) * inv_root).astype(
        jnp.bfloat16
    )
    inner_one = silu(matmul(base, w_res_v[0])).astype(jnp.bfloat16)
    middle = ((base.astype(jnp.float32) + silu(matmul(inner_one, w_res_v[1]))) * inv_root).astype(
        jnp.bfloat16
    )
    inner_two = silu(matmul(middle, w_res_v[2])).astype(jnp.bfloat16)
    chain_v[...] = (middle.astype(jnp.float32) + silu(matmul(inner_two, w_res_v[3]))) * inv_root
    sum_v[...] = jnp.zeros_like(sum_v)

    def some_tiles(group, carry):
        tiles = []
        for slot in range(expand_v.shape[0]):
            step = group * expand_v.shape[0] + slot
            tile = partner(me, step, n)
            tiles.append(tile)
            arrive(1, in_v, step, tile)
            arrive(2, out_v, step, tile)
            arrive(3, valid_v, step, tile)
            arrive(4, basis_v, step, tile)
        for slot, tile in enumerate(tiles):
            in_hot = hot_from(edge_count, look_up(send_v[tile], in_v[tile] & (cap - 1)))
            expand_v[slot] = matmul(table_v[...], in_hot)
            coeffs = basis_v[tile].astype(jnp.float32) * valid_v[tile].astype(jnp.float32)
            mixed = jnp.zeros((width, cap), jnp.float32)
            for k in range(basis_count):
                mixed = mixed + coeffs[k : k + 1, :] * expand_v[slot, k * width : (k + 1) * width, :]
            out_hot = hot_from(edge_count, look_up(return_v[tile], out_v[tile] & (cap - 1)))
            sum_v[...] += dot_at(mixed.astype(jnp.bfloat16), out_hot, 1, 1)
        return carry

    lax.fori_loop(0, n // expand_v.shape[0], some_tiles, 0)
    aggregate = sum_v[...].T.astype(jnp.bfloat16)
    update = silu(matmul(aggregate, w_up_v[...]))
    edge_out = (chain_v[...] + update).astype(jnp.bfloat16)
    edge_out_ref[...] = edge_out
    contrib = matmul(edge_out, w_atom_v[...]).astype(jnp.bfloat16)
    atom_sum = matmul(hot_columns(atom_v.shape[0], target_v[...]), contrib)
    atom_out_ref[...] = (atom_v[...].astype(jnp.float32) + silu(0.25 * atom_sum)).astype(
        jnp.bfloat16
    )
    for copy in sent:
        copy.wait_send()


def on_device(
    n,
    edge_state,
    atom_state,
    atom_sends,
    edge_source,
    edge_target,
    send_edges,
    triplet_in,
    triplet_out,
    triplet_valid,
    triplet_basis,
    return_edges,
    w_edge,
    w_source,
    w_down,
    w_bilinear,
    w_up,
    w_residual,
    w_atom,
):
    cap = triplet_in.shape[0] // n
    if cap % WIN or cap & (cap - 1) or n & (n - 1):
        return plain_on_device(
            edge_state,
            atom_state,
            atom_sends,
            edge_source,
            edge_target,
            send_edges,
            triplet_in,
            triplet_out,
            triplet_valid,
            triplet_basis,
            return_edges,
            w_edge,
            w_source,
            w_down,
            w_bilinear,
            w_up,
            w_residual,
            w_atom,
        )
    edge_count, edge_width = edge_state.shape
    atom_count, atom_width = atom_state.shape
    basis_count = triplet_basis.shape[0]
    width = w_down.shape[1]
    slots = atom_sends.shape[0] // n
    bf16 = jnp.bfloat16
    loaded = (
        atom_state,
        atom_sends.reshape(1, -1),
        edge_state,
        w_edge,
        edge_source.reshape(1, -1),
        w_source,
        w_down.T,
        w_bilinear,
        w_residual,
        send_edges.reshape(n, 1, cap),
        return_edges.reshape(n, 1, cap),
        edge_target.reshape(1, -1),
        w_up,
        w_atom,
    )
    group = 2 if n % 2 == 0 else 1
    return pl.pallas_call(
        functools.partial(block_kernel, n, len(loaded)),
        out_shape=(
            jax.ShapeDtypeStruct((edge_count, edge_width), bf16),
            jax.ShapeDtypeStruct((atom_count, atom_width), bf16),
        ),
        in_specs=[pl.BlockSpec(memory_space=pl.ANY)] * (len(loaded) + 4),
        out_specs=(pl.BlockSpec(memory_space=pltpu.VMEM),) * 2,
        scratch_shapes=[pltpu.VMEM(each.shape, each.dtype) for each in loaded]
        + [
            pltpu.VMEM((n, 1, cap), jnp.int32),
            pltpu.VMEM((n, 1, cap), jnp.int32),
            pltpu.VMEM((n, 1, cap), jnp.int32),
            pltpu.VMEM((n, basis_count, cap), bf16),
            pltpu.VMEM((n, slots, atom_width), bf16),
            pltpu.VMEM((n, slots, atom_width), bf16),
            pltpu.VMEM((edge_count, edge_width), jnp.float32),
            pltpu.VMEM((basis_count * width, edge_count), bf16),
            pltpu.VMEM((group, basis_count * width, cap), jnp.float32),
            pltpu.VMEM((width, edge_count), jnp.float32),
            pltpu.SemaphoreType.DMA((len(loaded),)),
            pltpu.SemaphoreType.DMA((5, n)),
            pltpu.SemaphoreType.DMA((5, n)),
        ],
        compiler_params=pltpu.CompilerParams(collective_id=0, has_side_effects=True),
        name="block",
    )(
        *loaded,
        triplet_in.reshape(n, 1, cap),
        triplet_out.reshape(n, 1, cap),
        triplet_valid.reshape(n, 1, cap),
        triplet_basis,
    )


def solution(mesh):
    placed = (
        P(("groups", "graph"), None),
        P(("groups", "graph"), None),
        P(("groups", "graph")),
        P(("groups", "graph")),
        P(("groups", "graph")),
        P(("groups", "graph")),
        P(("groups", "graph")),
        P(("groups", "graph")),
        P(("groups", "graph")),
        P(None, ("groups", "graph")),
        P(("groups", "graph")),
        P(),
        P(),
        P(),
        P(),
        P(),
        P(),
        P(),
    )
    return jax.shard_map(
        functools.partial(on_device, mesh.shape["graph"]),
        mesh=mesh,
        in_specs=placed,
        out_specs=(P(("groups", "graph"), None), P(("groups", "graph"), None)),
        check_vma=False,
    )
```

```python
import functools

import jax
import jax.numpy as jnp
from jax import lax
from jax.experimental import pallas as pl
from jax.experimental.pallas import tpu as pltpu
from jax.sharding import PartitionSpec as P

WIN = 512


inv_root = 0.7071067811865476


def matmul(left, right):
    return jnp.dot(left, right, preferred_element_type=jnp.float32)


def pick_rows(indices, table):
    chooser = (indices[:, None] == jnp.arange(table.shape[0], dtype=jnp.int32)[None, :]).astype(
        table.dtype
    )
    return matmul(chooser, table).astype(table.dtype)


def bilinear_terms(inputs_x, coeffs, keeps, w_bilinear):
    expanded = matmul(inputs_x, w_bilinear)
    expanded = expanded.reshape(inputs_x.shape[0], coeffs.shape[0], -1)
    mixed = jnp.einsum("tkd,kt->td", expanded, coeffs.astype(jnp.float32))
    return mixed * keeps.astype(jnp.float32)[:, None]


def tile_sums(slot_rows, local_in, local_out, keeps, coeffs, w_bilinear):
    trip_count = slot_rows.shape[0]
    block_size = WIN
    block_count = trip_count // block_size
    basis_rows = coeffs.shape[0]
    block_iota = jnp.arange(block_size, dtype=jnp.int32)

    def one_block(operands):
        rows_blk, in_blk, out_blk, keep_blk, coef_blk = operands
        in_hot = ((in_blk % block_size)[:, None] == block_iota[None, :]).astype(jnp.bfloat16)
        inputs_x = matmul(in_hot, rows_blk).astype(jnp.bfloat16)
        mixed = bilinear_terms(inputs_x, coef_blk, keep_blk, w_bilinear)
        out_hot = (block_iota[:, None] == (out_blk % block_size)[None, :]).astype(jnp.float32)
        return jnp.dot(
            out_hot, mixed, precision=lax.Precision.HIGHEST, preferred_element_type=jnp.float32
        )

    shaped_coeffs = jnp.transpose(coeffs.reshape(basis_rows, block_count, block_size), (1, 0, 2))
    summed = lax.map(
        one_block,
        (
            slot_rows.reshape(block_count, block_size, -1),
            local_in.reshape(block_count, block_size),
            local_out.reshape(block_count, block_size),
            keeps.reshape(block_count, block_size),
            shaped_coeffs,
        ),
    )
    return summed.reshape(trip_count, -1).astype(jnp.bfloat16)


def plain_on_device(
    edge_state,
    atom_state,
    atom_sends,
    edge_source,
    edge_target,
    send_edges,
    triplet_in,
    triplet_out,
    triplet_valid,
    triplet_basis,
    return_edges,
    w_edge,
    w_source,
    w_down,
    w_bilinear,
    w_up,
    w_residual,
    w_atom,
):
    edge_count = edge_state.shape[0]
    atom_count = atom_state.shape[0]
    arrived_atoms = lax.all_to_all(
        pick_rows(atom_sends, atom_state), "graph", split_axis=0, concat_axis=0, tiled=True
    )
    src_rows = pick_rows(edge_source, arrived_atoms)
    pre_act = matmul(edge_state, w_edge) + matmul(src_rows, w_source)
    activated = jax.nn.silu(pre_act).astype(jnp.bfloat16)
    projected = jax.nn.silu(matmul(activated, w_down)).astype(jnp.bfloat16)
    slot_rows = lax.all_to_all(
        pick_rows(send_edges, projected), "graph", split_axis=0, concat_axis=0, tiled=True
    )
    slot_sums = tile_sums(
        slot_rows, triplet_in, triplet_out, triplet_valid, triplet_basis, w_bilinear
    )
    returned = lax.all_to_all(slot_sums, "graph", split_axis=0, concat_axis=0, tiled=True)
    back_hot = (jnp.arange(edge_count, dtype=jnp.int32)[:, None] == return_edges[None, :]).astype(
        jnp.bfloat16
    )
    aggregate = matmul(back_hot, returned)
    update = jax.nn.silu(matmul(aggregate.astype(jnp.bfloat16), w_up))
    base = ((edge_state.astype(jnp.float32) + activated.astype(jnp.float32)) * inv_root).astype(
        jnp.bfloat16
    )
    inner_one = jax.nn.silu(matmul(base, w_residual[0])).astype(jnp.bfloat16)
    middle = (
        (base.astype(jnp.float32) + jax.nn.silu(matmul(inner_one, w_residual[1]))) * inv_root
    ).astype(jnp.bfloat16)
    inner_two = jax.nn.silu(matmul(middle, w_residual[2])).astype(jnp.bfloat16)
    chain = (middle.astype(jnp.float32) + jax.nn.silu(matmul(inner_two, w_residual[3]))) * inv_root
    edge_out = (chain + update).astype(jnp.bfloat16)
    contrib = matmul(edge_out, w_atom).astype(jnp.bfloat16)
    one_hot = (edge_target[None, :] == jnp.arange(atom_count, dtype=jnp.int32)[:, None]).astype(
        jnp.bfloat16
    )
    atom_sum = matmul(one_hot, contrib)
    atom_out = (atom_state.astype(jnp.float32) + jax.nn.silu(0.25 * atom_sum)).astype(jnp.bfloat16)
    return (edge_out, atom_out)


def silu(value):
    return value / (1.0 + jnp.exp(-value))


def dot_at(left, right, left_dim, right_dim):
    return lax.dot_general(
        left, right, (((left_dim,), (right_dim,)), ((), ())), preferred_element_type=jnp.float32
    )


def hot_columns(row_count, indices):
    rows = lax.broadcasted_iota(jnp.int32, (row_count, indices.shape[1]), 0)
    return jnp.where(rows == indices, 1.0, 0.0).astype(jnp.bfloat16)


def partner(me, step, n):
    peer = me
    bit = 1
    while bit < n:
        mine = lax.rem(lax.div(me, bit), 2)
        flip = (step // bit) % 2 if isinstance(step, int) else lax.rem(lax.div(step, bit), 2)
        peer = peer + flip * (1 - 2 * mine) * bit
        bit *= 2
    return peer


def look_up(table, indices):
    lanes = 128
    found = []
    for start in range(0, indices.shape[1], lanes):
        wanted = jnp.broadcast_to(indices[:, start : start + lanes], (8, lanes))
        lane = wanted & (lanes - 1)
        value = jnp.zeros_like(wanted)
        for first in range(0, table.shape[1], lanes):
            part = jnp.take_along_axis(
                jnp.broadcast_to(table[:, first : first + lanes], (8, lanes)),
                lane,
                axis=1,
                mode="promise_in_bounds",
            )
            value = jnp.where(wanted - lane == first, part, value)
        found.append(value)
    return jnp.concatenate(found, axis=1)


def hot_from(row_count, eight_rows):
    rows = lax.broadcasted_iota(jnp.int32, (row_count, eight_rows.shape[1]), 0)
    spread = jnp.concatenate([eight_rows] * (row_count // 8), axis=0)
    return jnp.where(rows == spread, 1.0, 0.0).astype(jnp.bfloat16)


def tail_kernel(sum_v, chain_v, atom_v, target_v, w_up_v, w_atom_v, edge_out_ref, atom_out_ref):
    aggregate = sum_v[...].T.astype(jnp.bfloat16)
    update = silu(matmul(aggregate, w_up_v[...]))
    edge_out = (chain_v[...] + update).astype(jnp.bfloat16)
    edge_out_ref[...] = edge_out
    contrib = matmul(edge_out, w_atom_v[...]).astype(jnp.bfloat16)
    atom_sum = matmul(hot_columns(atom_v.shape[0], target_v[...]), contrib)
    atom_out_ref[...] = (atom_v[...].astype(jnp.float32) + silu(0.25 * atom_sum)).astype(
        jnp.bfloat16
    )


def block_kernel(n, loaded, *refs):
    sources = refs[:loaded]
    in_hbm, out_hbm, valid_hbm, basis_hbm = refs[loaded : loaded + 4]
    chain_v, sum_v = refs[loaded + 4 : loaded + 6]
    held = refs[loaded + 6 : 2 * loaded + 6]
    (
        stage_v,
        ends_v,
        stage_basis_v,
        basis_v,
        atoms_out,
        atoms_in,
        table_v,
        expand_v,
        load_sem,
        stage_sem,
        send_sem,
        recv_sem,
    ) = refs[2 * loaded + 6 :]
    (
        atom_v,
        asend_v,
        edge_v,
        w_edge_v,
        source_v,
        w_source_v,
        w_down_v,
        w_bilinear_v,
        w_res_v,
        send_v,
        return_v,
    ) = held
    me = lax.axis_index("graph")
    cap = ends_v.shape[3]
    edge_count = edge_v.shape[0]
    width = w_down_v.shape[0]
    basis_count = basis_v.shape[1]

    barrier = pltpu.get_barrier_semaphore()
    for step in range(1, n):
        pl.semaphore_signal(
            barrier,
            inc=1,
            device_id={"graph": partner(me, step, n)},
            device_id_type=pl.DeviceIdType.MESH,
        )
    loads = [
        pltpu.make_async_copy(src, dst, load_sem.at[i])
        for i, (src, dst) in enumerate(zip(sources, held))
    ]
    for load in loads:
        load.start()
    stages = [
        pltpu.make_async_copy(src, stage_v.at[:, i], stage_sem.at[i])
        for i, src in enumerate((in_hbm, out_hbm, valid_hbm))
    ]
    stages.append(pltpu.make_async_copy(basis_hbm, stage_basis_v, stage_sem.at[3]))
    for stage in stages:
        stage.start()
    loads[0].wait()
    loads[1].wait()
    picked = dot_at(hot_columns(atom_v.shape[0], asend_v[...]), atom_v[...], 0, 0)
    atoms_out[...] = picked.reshape(atoms_out.shape).astype(jnp.bfloat16)
    pl.semaphore_wait(barrier, n - 1)

    def parts(peer):
        lanes = pl.ds(pl.multiple_of(peer * cap, cap), cap)
        return (
            (atoms_out.at[peer], atoms_in.at[me]),
            (stage_v.at[peer], ends_v.at[me]),
            (stage_basis_v.at[:, lanes], basis_v.at[me]),
        )

    sent = []
    for kinds in ((0,), (1, 2)):
        if kinds[0]:
            for stage in stages:
                stage.wait()
        for step in range(n):
            peer = partner(me, step, n)
            for kind in kinds:
                src, dst = parts(peer)[kind]
                if step == 0:
                    copy = pltpu.make_async_copy(src, dst, recv_sem.at[kind, step])
                else:
                    copy = pltpu.make_async_remote_copy(
                        src_ref=src,
                        dst_ref=dst,
                        send_sem=send_sem.at[kind, step],
                        recv_sem=recv_sem.at[kind, step],
                        device_id={"graph": peer},
                        device_id_type=pl.DeviceIdType.MESH,
                    )
                    sent.append(copy)
                copy.start()

    def arrive(kind, buffer, step, peer):
        pltpu.make_async_copy(buffer.at[peer], buffer.at[peer], recv_sem.at[kind, step]).wait()

    for load in loads[2:7]:
        load.wait()
    edge = edge_v[...]
    pre_act = matmul(edge, w_edge_v[...])
    pick = hot_columns(atoms_in.shape[0] * atoms_in.shape[1], source_v[...])
    for step in range(n):
        arrive(0, atoms_in, step, partner(me, step, n))
    arrived = atoms_in[...].astype(jnp.float32).reshape(pick.shape[0], -1).astype(jnp.bfloat16)
    src_rows = dot_at(pick, arrived, 0, 0).astype(jnp.bfloat16)
    activated = silu(pre_act + matmul(src_rows, w_source_v[...])).astype(jnp.bfloat16)
    projected = silu(dot_at(activated, w_down_v[...], 1, 1)).astype(jnp.bfloat16)
    for load in loads[7:]:
        load.wait()
    table_v[...] = dot_at(w_bilinear_v[...], projected, 0, 1).astype(jnp.bfloat16)
    base = ((edge.astype(jnp.float32) + activated.astype(jnp.float32)) * inv_root).astype(
        jnp.bfloat16
    )
    inner_one = silu(matmul(base, w_res_v[0])).astype(jnp.bfloat16)
    middle = ((base.astype(jnp.float32) + silu(matmul(inner_one, w_res_v[1]))) * inv_root).astype(
        jnp.bfloat16
    )
    inner_two = silu(matmul(middle, w_res_v[2])).astype(jnp.bfloat16)
    chain_v[...] = (middle.astype(jnp.float32) + silu(matmul(inner_two, w_res_v[3]))) * inv_root
    sum_v[...] = jnp.zeros_like(sum_v)

    def some_tiles(group, carry):
        tiles = []
        for slot in range(expand_v.shape[0]):
            step = group * expand_v.shape[0] + slot
            tile = partner(me, step, n)
            tiles.append(tile)
            arrive(1, ends_v, step, tile)
            arrive(2, basis_v, step, tile)
        for slot, tile in enumerate(tiles):
            in_hot = hot_from(edge_count, look_up(send_v[tile], ends_v[tile, 0] & (cap - 1)))
            expand_v[slot] = matmul(table_v[...], in_hot)
            coeffs = basis_v[tile].astype(jnp.float32) * ends_v[tile, 2].astype(jnp.float32)
            mixed = jnp.zeros((width, cap), jnp.float32)
            for k in range(basis_count):
                mixed = mixed + coeffs[k : k + 1, :] * expand_v[slot, k * width : (k + 1) * width, :]
            out_hot = hot_from(edge_count, look_up(return_v[tile], ends_v[tile, 1] & (cap - 1)))
            sum_v[...] += dot_at(mixed.astype(jnp.bfloat16), out_hot, 1, 1)
        return carry

    lax.fori_loop(0, n // expand_v.shape[0], some_tiles, 0)
    for copy in sent:
        copy.wait_send()


def on_device(
    n,
    edge_state,
    atom_state,
    atom_sends,
    edge_source,
    edge_target,
    send_edges,
    triplet_in,
    triplet_out,
    triplet_valid,
    triplet_basis,
    return_edges,
    w_edge,
    w_source,
    w_down,
    w_bilinear,
    w_up,
    w_residual,
    w_atom,
):
    cap = triplet_in.shape[0] // n
    if cap % WIN or cap & (cap - 1) or n & (n - 1):
        return plain_on_device(
            edge_state,
            atom_state,
            atom_sends,
            edge_source,
            edge_target,
            send_edges,
            triplet_in,
            triplet_out,
            triplet_valid,
            triplet_basis,
            return_edges,
            w_edge,
            w_source,
            w_down,
            w_bilinear,
            w_up,
            w_residual,
            w_atom,
        )
    edge_count, edge_width = edge_state.shape
    atom_count, atom_width = atom_state.shape
    basis_count = triplet_basis.shape[0]
    width = w_down.shape[1]
    slots = atom_sends.shape[0] // n
    bf16 = jnp.bfloat16
    loaded = (
        atom_state,
        atom_sends.reshape(1, -1),
        edge_state,
        w_edge,
        edge_source.reshape(1, -1),
        w_source,
        w_down.T,
        w_bilinear,
        w_residual,
        send_edges.reshape(n, 1, cap),
        return_edges.reshape(n, 1, cap),
    )
    group = 4 if n % 4 == 0 else 1
    chain, total = pl.pallas_call(
        functools.partial(block_kernel, n, len(loaded)),
        out_shape=(
            jax.ShapeDtypeStruct((edge_count, edge_width), jnp.float32),
            jax.ShapeDtypeStruct((width, edge_count), jnp.float32),
        ),
        in_specs=[pl.BlockSpec(memory_space=pl.ANY)] * (len(loaded) + 4),
        out_specs=(pl.BlockSpec(memory_space=pltpu.VMEM),) * 2,
        scratch_shapes=[pltpu.VMEM(each.shape, each.dtype) for each in loaded]
        + [
            pltpu.VMEM((n, 3, 1, cap), jnp.int32),
            pltpu.VMEM((n, 3, 1, cap), jnp.int32),
            pltpu.VMEM(triplet_basis.shape, bf16),
            pltpu.VMEM((n, basis_count, cap), bf16),
            pltpu.VMEM((n, slots, atom_width), bf16),
            pltpu.VMEM((n, slots, atom_width), bf16),
            pltpu.VMEM((basis_count * width, edge_count), bf16),
            pltpu.VMEM((group, basis_count * width, cap), jnp.float32),
            pltpu.SemaphoreType.DMA((len(loaded),)),
            pltpu.SemaphoreType.DMA((4,)),
            pltpu.SemaphoreType.DMA((3, n)),
            pltpu.SemaphoreType.DMA((3, n)),
        ],
        compiler_params=pltpu.CompilerParams(collective_id=0, has_side_effects=True),
        name="block",
    )(
        *loaded,
        triplet_in.reshape(n, 1, cap),
        triplet_out.reshape(n, 1, cap),
        triplet_valid.reshape(n, 1, cap),
        triplet_basis,
    )
    return pl.pallas_call(
        tail_kernel,
        out_shape=(
            jax.ShapeDtypeStruct((edge_count, edge_width), bf16),
            jax.ShapeDtypeStruct((atom_count, atom_width), bf16),
        ),
        in_specs=[pl.BlockSpec(memory_space=pltpu.VMEM)] * 6,
        out_specs=(pl.BlockSpec(memory_space=pltpu.VMEM),) * 2,
        name="tail",
    )(total, chain, atom_state, edge_target.reshape(1, -1), w_up, w_atom)


def solution(mesh):
    placed = (
        P(("groups", "graph"), None),
        P(("groups", "graph"), None),
        P(("groups", "graph")),
        P(("groups", "graph")),
        P(("groups", "graph")),
        P(("groups", "graph")),
        P(("groups", "graph")),
        P(("groups", "graph")),
        P(("groups", "graph")),
        P(None, ("groups", "graph")),
        P(("groups", "graph")),
        P(),
        P(),
        P(),
        P(),
        P(),
        P(),
        P(),
    )
    return jax.shard_map(
        functools.partial(on_device, mesh.shape["graph"]),
        mesh=mesh,
        in_specs=placed,
        out_specs=(P(("groups", "graph"), None), P(("groups", "graph"), None)),
        check_vma=False,
    )
```
